8 devices in a mesh: dp: 2 (over y, z), ep: 4 (over x, core).
Axes of the slice: x: 2, y: 2, z: 1, core: 2. Of those that a mesh axis runs over, the one named last changes fastest.
Arguments:
- x: bfloat16 [2, 4, 256, 6144], P('dp', 'ep'), parts along dimension 0
- expert: int32 [2, 4, 256, 4], P('dp', 'ep'), parts along dimension 0
- slot: int32 [2, 4, 256, 4], P('dp', 'ep'), parts along dimension 0
- gate: float32 [2, 4, 256, 4], P('dp', 'ep'), parts along dimension 0
- w_gate: bfloat16 [8, 6144, 10752], P('ep')
- w_up: bfloat16 [8, 6144, 10752], P('ep')
- w_down: bfloat16 [8, 10752, 6144], P('ep')
Outputs:
- y: bfloat16 [2, 4, 256, 6144], P('dp', 'ep'), parts along dimension 0
There are 2 independent parts. The reference program is written for one: setup_inputs(seed, part) draws one part's arguments, and reference() takes and returns one part's arrays. A program takes and returns all parts, laid end to end along the dimension named above; an argument that names none is the same for every part.
All inputs are finite; a program needn't handle non-finite values.
Results may differ from the reference program's by a relative error of at most 0.009.
Values are sent between devices in bfloat16 or wider.
A program may use at most 2 GiB of HBM per device.

```python
import jax
import jax.numpy as jnp

MEMBERS = 4
TOKENS = 256
D = 6144
FF = 10752
TOP = 4
EXPERTS = 8
SLOTS = 5 * TOKENS * TOP // (4 * EXPERTS)


def setup_inputs(seed: int = 0, part: int = 0) -> dict:
    own, k1, k2, k3, k4, k5, k6 = jax.random.split(jax.random.key(seed), 7)
    kx, ke, kl, kg = jax.random.split(jax.random.fold_in(own, part), 4)
    devices = (1, MEMBERS)
    place = jax.random.permutation(kl, jnp.arange(EXPERTS, dtype=jnp.uint32))
    slow = ((EXPERTS + (9 * place) % EXPERTS) << ((9 * place) // EXPERTS)) // EXPERTS
    wait = (jax.random.bits(ke, (*devices, TOKENS, EXPERTS), jnp.uint32) >> 10) * slow
    expert = jnp.argsort(wait, axis=-1)[..., :TOP].astype(jnp.int32)
    chosen = jax.nn.one_hot(expert, EXPERTS, dtype=jnp.int32)
    in_line = jnp.cumsum(chosen.reshape(*devices, TOKENS * TOP, EXPERTS), axis=2) - 1
    slot = jnp.sum(in_line.reshape(chosen.shape) * chosen, axis=-1)

    def one(key, rows, columns):
        return (jax.random.normal(key, (rows, columns), jnp.float32) * rows**-0.5).astype(jnp.bfloat16)

    def weights(key, rows, columns):
        return jax.lax.map(lambda k: one(k, rows, columns), jax.random.split(key, EXPERTS))

    return {
        "x": jax.random.normal(kx, (*devices, TOKENS, D), jnp.float32).astype(jnp.bfloat16),
        "expert": expert,
        "slot": slot,
        "gate": jax.nn.softmax(jax.random.normal(kg, expert.shape, jnp.float32)),
        "w_gate": weights(k1, D, FF),
        "w_up": weights(k2, D, FF),
        "w_down": weights(k3, FF, D),
    }


def einsum(form, a, b):
    return jnp.einsum(form, a.astype(jnp.float32), b.astype(jnp.float32))


def reference(x, expert, slot, gate, w_gate, w_up, w_down):
    to_expert = jax.nn.one_hot(expert, EXPERTS, dtype=jnp.bfloat16)
    to_slot = jax.nn.one_hot(slot, SLOTS, dtype=jnp.bfloat16)
    weighted = to_expert * gate[..., None].astype(jnp.bfloat16)
    dispatch = einsum("abtke,abtkc->abtec", to_expert, to_slot).astype(jnp.bfloat16)
    combine = einsum("abtke,abtkc->abtec", weighted, to_slot).astype(jnp.bfloat16)
    z = einsum("abtec,abtd->aebcd", dispatch, x).astype(jnp.bfloat16)
    h = jax.nn.silu(einsum("aebcd,edf->aebcf", z, w_gate))
    h = (h * einsum("aebcd,edf->aebcf", z, w_up)).astype(jnp.bfloat16)
    out = einsum("aebcf,efd->aebcd", h, w_down).astype(jnp.bfloat16)
    y = einsum("abtec,aebcd->abtd", combine, out)
    return y.astype(jnp.bfloat16)
```

```python
import functools

import jax
import jax.numpy as jnp
from jax import lax
from jax.experimental import pallas as pl
from jax.experimental.pallas import tpu as pltpu
from jax.sharding import PartitionSpec as P


F32, BF16, I32 = jnp.float32, jnp.bfloat16, jnp.int32
MESH = pl.DeviceIdType.MESH
VMEM_LIMIT = 62 * 2**20
CHUNKS = (1536, 1536, 1536, 1024, 512)
NEAR_BLOCK, REST_BLOCK, DOWN_BLOCK = 512, 512, 256
NEAR_SIZES = (192, 256, 320)
NEAR_STEPS = 15
ROW_CHUNKS = (192, 224, 256, 288, 320)
SOURCES = 6
FIRST, SECOND, NEAR, ROWS, START, COUNT = 0, 1, 2, 3, 8, 24


def cost(flops, nbytes):
    return pl.CostEstimate(flops=int(flops), bytes_accessed=int(nbytes), transcendentals=0)


def plan_kernel(slots, expert_ref, slot_ref, gate_ref, pos_ref, scale_ref, num_ref, mine, got, send, recv):
    dp, ep = lax.axis_index("dp"), lax.axis_index("ep")
    tokens = expert_ref.shape[1]

    def peer(i):
        return (dp ^ (i // 4), ep ^ (i % 4))

    expert, slot = expert_ref[...], slot_ref[...]
    gate = gate_ref[...].astype(BF16).astype(F32)
    for pair in range(4):
        rows = []
        for e in (2 * pair, 2 * pair + 1):
            hit = (expert == e) & (slot < slots)
            rows.append(jnp.sum(jnp.where(hit, 1.0, 0.0), 0, keepdims=True))
            rows.append(jnp.sum(jnp.where(hit, gate, 0.0), 0, keepdims=True))
        rows = [rows[0], rows[2], rows[1], rows[3], jnp.zeros((4, tokens), F32)]
        mine[pair] = jnp.concatenate(rows, 0)

    barrier = pltpu.get_barrier_semaphore()
    for i in range(1, 8):
        pl.semaphore_signal(barrier, inc=1, device_id=peer(i), device_id_type=MESH)
    pl.semaphore_wait(barrier, 7)
    copies = []
    for i in range(1, 8):
        copies.append(
            pltpu.make_async_remote_copy(
                src_ref=mine.at[ep ^ (i % 4)],
                dst_ref=got.at[i],
                send_sem=send.at[i],
                recv_sem=recv.at[i],
                device_id=peer(i),
                device_id_type=MESH,
            )
        )
    for copy in copies:
        copy.start()
    for copy in copies:
        copy.wait()

    blocks = [mine[ep]] + [got[i] for i in range(1, 8)]
    valid = jnp.concatenate([b[0:2] for b in blocks], 0)
    scales = [b[2:4] for b in blocks]
    upper = lax.broadcasted_iota(I32, (tokens, tokens), 0) <= lax.broadcasted_iota(I32, (tokens, tokens), 1)
    upto = jnp.dot(valid.astype(BF16), upper.astype(F32).astype(BF16), preferred_element_type=F32)

    results = []
    for e in range(2):
        v = [valid[2 * i + e : 2 * i + e + 1] > 0.0 for i in range(8)]
        rank = [upto[2 * i + e : 2 * i + e + 1] - 1.0 for i in range(8)]
        c = [r[:, tokens - 1 :] + 1.0 for r in rank]
        near, other = c[0] + c[1], c[4] + c[5]
        gap = near + c[2] + c[3] - other - c[6] - c[7]
        give = jnp.minimum(jnp.maximum(jnp.floor(gap * 0.5), 0.0), near)
        take = jnp.minimum(jnp.maximum(jnp.floor(-gap * 0.5), 0.0), other)
        keep, skip = near - give, other - take
        counts = [jnp.minimum(c[0], keep)]
        counts += [keep - counts[0], c[2], c[3], jnp.maximum(c[4] - skip, 0.0)]
        counts += [take - counts[4]]
        starts = [jnp.zeros_like(keep)]
        for n in counts:
            starts.append(starts[-1] + n)
        place = [rank[0], rank[1] + c[0], rank[2] + starts[2], rank[3] + starts[3]]
        mine_too = [v[0] & (place[0] < keep), v[1] & (place[1] < keep), v[2], v[3]]
        for i, n in ((4, rank[4]), (5, rank[5] + c[4])):
            mine_too.append(v[i] & (n >= skip))
            place.append(n - skip + starts[4])
        pos = [jnp.where(m, p, -1.0) for m, p in zip(mine_too, place)]
        results.append((keep, starts[6], starts[:6], counts, pos, [s[e : e + 1] for s in scales[:6]]))

    swap = results[1][0] > results[0][0]

    def pick(a, b):
        return jnp.where(swap, b, a), jnp.where(swap, a, b)

    (a_keep, a_rows, a_starts, a_counts, a_pos, a_scale), (b_keep, b_rows, b_starts, b_counts, b_pos, b_scale) = results
    pad = jnp.full((2, tokens), -1.0, F32)
    pos = [pick(a, b) for a, b in zip(a_pos, b_pos)]
    scale = [pick(a, b) for a, b in zip(a_scale, b_scale)]
    pos_ref[...] = jnp.concatenate([p[0] for p in pos] + [pad] + [p[1] for p in pos] + [pad], 0).astype(I32)
    scale_ref[...] = jnp.concatenate([p[0] for p in scale] + [pad] + [p[1] for p in scale] + [pad], 0)
    lane = lax.broadcasted_iota(I32, (1, 128), 1)
    numbers = {FIRST: jnp.where(swap, 1.0, 0.0), SECOND: jnp.where(swap, 0.0, 1.0)}
    numbers[NEAR] = pick(a_keep, b_keep)[0]
    numbers[ROWS], numbers[ROWS + 1] = pick(a_rows, b_rows)
    for s in range(SOURCES):
        numbers[START + s], numbers[START + 8 + s] = pick(a_starts[s], b_starts[s])
        numbers[COUNT + s], numbers[COUNT + 8 + s] = pick(a_counts[s], b_counts[s])
    out = jnp.zeros((1, 128), F32)
    for at, value in numbers.items():
        out = jnp.where(lane == at, value, out)
    num_ref[...] = out.astype(I32)


def plan(expert, slot, gate, slots):
    tokens = expert.shape[1]
    return pl.pallas_call(
        functools.partial(plan_kernel, slots),
        out_shape=[
            jax.ShapeDtypeStruct((16, tokens), I32),
            jax.ShapeDtypeStruct((16, tokens), F32),
            jax.ShapeDtypeStruct((1, 128), I32),
        ],
        scratch_shapes=[
            pltpu.VMEM((4, 8, tokens), F32),
            pltpu.VMEM((8, 8, tokens), F32),
            pltpu.SemaphoreType.DMA((8,)),
            pltpu.SemaphoreType.DMA((8,)),
        ],
        cost_estimate=cost(10**7, 10**5),
        compiler_params=pltpu.CompilerParams(collective_id=0, has_side_effects=True),
        name="plan",
    )(expert, slot, gate)


def floor16(n):
    return n // 16 * 16


def place_rows(window, x_ref, pos, start, count, z_ref, block=2048):
    tokens, d = x_ref.shape
    low = pl.multiple_of(floor16(start), 16)

    @pl.when(count > 0)
    def _():
        rows = lax.broadcasted_iota(I32, (window, tokens), 0) + low
        pick = (rows == pos).astype(F32).astype(BF16)

        def step(k, _):
            at = pl.ds(pl.multiple_of(k * block, block), block)
            z = jnp.dot(pick, x_ref[:, at], preferred_element_type=F32).astype(BF16)
            z_ref[pl.ds(low, 16), at] += z[:16]
            z_ref[pl.ds(pl.multiple_of(low + 16, 16), window - 16), at] = z[16:]
            return 0

        lax.fori_loop(0, d // block, step, 0)


def sizes_do(sizes, n, body):
    for k, size in enumerate(sizes):
        low = n > sizes[k - 1] if k else n >= 0
        high = n <= size if k + 1 < len(sizes) else n >= 0
        pl.when(low & high)(functools.partial(body, size))


def chunks_do(rows, body):
    single = [c for c in ROW_CHUNKS if c % 64 == 0]
    for c in ROW_CHUNKS:
        two = (rows > max(2 * c - 64, ROW_CHUNKS[-1])) & (rows <= 2 * c)
        use = two
        if c in single:
            k = single.index(c)
            use = two | ((rows > (single[k - 1] if k else -1)) & (rows <= c))
        pl.when(use)(functools.partial(body, c, jnp.where(two, 2, 1)))


def swiglu(z, wg, wu):
    g = jnp.dot(z, wg, preferred_element_type=F32)
    u = jnp.dot(z, wu, preferred_element_type=F32)
    return (jax.nn.silu(g) * u).astype(BF16)


def up_near_kernel(window, num, x_ref, mate_ref, pos_ref, scale_ref, wg_ref, wu_ref, h_ref, mix_ref, z):
    j = pl.program_id(0)
    tokens = x_ref.shape[0]

    @pl.when((j > 0) & (j <= 2 * SOURCES))
    def _():
        k = j - 1
        row = k // SOURCES * 8 + lax.rem(k, SOURCES)
        at = lax.broadcasted_iota(I32, (window, tokens), 0) + floor16(num[START + row])
        weight = jnp.where(at == pos_ref[pl.ds(row, 1), :], scale_ref[pl.ds(row, 1), :], 0.0)
        mix_ref[k] = weight.T.astype(BF16)

    @pl.when(j == 0)
    def _():
        z[...] = jnp.zeros_like(z)
        for s, ref in enumerate((x_ref, mate_ref)):
            place_rows(window, ref, pos_ref[s : s + 1, :], num[START + s], num[COUNT + s], z)

    def body(m):
        h_ref[0:m] = swiglu(z[0:m], wg_ref[...], wu_ref[...])
        if m < h_ref.shape[0]:
            h_ref[m:] = jnp.zeros((h_ref.shape[0] - m, h_ref.shape[1]), BF16)

    sizes_do(NEAR_SIZES, num[NEAR], body)


def up_near(num, x, mate, pos, scale, wg, wu, slots):
    tokens, d = x.shape
    window, rows = slots + 16, NEAR_SIZES[-1]
    whole = pl.BlockSpec((tokens, d), lambda j, num: (0, 0), pipeline_mode=pl.Buffered(1))
    weights = pl.BlockSpec((None, d, NEAR_BLOCK), lambda j, num: (num[FIRST], 0, j))
    return pl.pallas_call(
        functools.partial(up_near_kernel, window),
        out_shape=[
            jax.ShapeDtypeStruct((rows, NEAR_STEPS * NEAR_BLOCK), BF16),
            jax.ShapeDtypeStruct((2 * SOURCES, tokens, window), BF16),
        ],
        grid_spec=pltpu.PrefetchScalarGridSpec(
            num_scalar_prefetch=1,
            grid=(NEAR_STEPS,),
            in_specs=[whole, whole]
            + [pl.BlockSpec(pos.shape, lambda j, num: (0, 0))] * 2
            + [weights, weights],
            out_specs=[
                pl.BlockSpec((rows, NEAR_BLOCK), lambda j, num: (0, j)),
                pl.BlockSpec((2 * SOURCES, tokens, window), lambda j, num: (0, 0, 0)),
            ],
            scratch_shapes=[pltpu.VMEM((rows + window, d), BF16)],
        ),
        cost_estimate=cost(4 * rows * d * NEAR_STEPS * NEAR_BLOCK, 4 * d * NEAR_STEPS * NEAR_BLOCK),
        compiler_params=pltpu.CompilerParams(vmem_limit_bytes=VMEM_LIMIT),
        name="up_near",
    )(num, x, mate, pos, scale, wg, wu)


def up_rest_kernel(window, steps, num, *refs):
    sources, (pos_ref, near_ref, wg_ref, wu_ref, one_ref, two_ref), xs = (
        refs[:SOURCES],
        refs[SOURCES : SOURCES + 6],
        refs[SOURCES + 6 : 2 * SOURCES + 6],
    )
    z, sems = refs[2 * SOURCES + 6 :]
    j = pl.program_id(0)
    copies = [pltpu.make_async_copy(sources[s], xs[s], sems.at[s]) for s in range(SOURCES)]

    def fill(e, fresh):
        z[...] = jnp.zeros_like(z)
        for s in range(SOURCES):
            if fresh:
                copies[s].wait()
            row = 8 * e + s
            place_rows(window, xs[s], pos_ref[row : row + 1, :], num[START + row], num[COUNT + row], z)

    @pl.when(j == 0)
    def _():
        for copy in copies:
            copy.start()
        fill(0, True)

    @pl.when(j == steps)
    def _():
        fill(1, False)

    near_rows = near_ref.shape[0]
    first = j < steps
    base = jnp.where(j < NEAR_STEPS, floor16(num[NEAR]), 0)
    rows = jnp.where(first, num[ROWS] - base, num[ROWS + 1])

    @pl.when(first)
    def _():
        one_ref[0:near_rows] = near_ref[...]
        one_ref[near_rows:] = jnp.zeros((one_ref.shape[0] - near_rows, one_ref.shape[1]), BF16)

    @pl.when(jnp.logical_not(first))
    def _():
        two_ref[...] = jnp.zeros_like(two_ref)

    def body(c, n):
        def chunk(t, _):
            at = pl.ds(pl.multiple_of(base + t * c, 16), c)
            h = swiglu(z[at], wg_ref[...], wu_ref[...])

            @pl.when(first)
            def _():
                one_ref[at] = h

            @pl.when(jnp.logical_not(first))
            def _():
                two_ref[at] = h

            return 0

        lax.fori_loop(0, n, chunk, 0)

    chunks_do(rows, body)


def up_rest(num, sources, pos, near, wg, wu, slots):
    tokens, d = sources[0].shape
    ff = wg.shape[2]
    window, rows = slots + 16, 2 * ROW_CHUNKS[-1]
    steps = ff // REST_BLOCK
    weights = pl.BlockSpec(
        (None, d, REST_BLOCK),
        lambda j, num: (jnp.where(j < steps, num[FIRST], num[SECOND]), 0, lax.rem(j, steps)),
    )
    early = lambda j, num: (0, jnp.minimum(j, steps - 1))
    late = lambda j, num: (0, jnp.maximum(j - steps, 0))
    return pl.pallas_call(
        functools.partial(up_rest_kernel, window, steps),
        out_shape=[jax.ShapeDtypeStruct((rows + 128, ff), BF16), jax.ShapeDtypeStruct((rows, ff), BF16)],
        grid_spec=pltpu.PrefetchScalarGridSpec(
            num_scalar_prefetch=1,
            grid=(2 * steps,),
            in_specs=[pl.BlockSpec(memory_space=pl.ANY)] * SOURCES
            + [
                pl.BlockSpec(pos.shape, lambda j, num: (0, 0)),
                pl.BlockSpec((near.shape[0], REST_BLOCK), lambda j, num: (0, jnp.minimum(j, NEAR_STEPS - 1))),
                weights,
                weights,
            ],
            out_specs=[pl.BlockSpec((rows + 128, REST_BLOCK), early), pl.BlockSpec((rows, REST_BLOCK), late)],
            scratch_shapes=[pltpu.VMEM((tokens, d), BF16)] * SOURCES
            + [pltpu.VMEM((rows + window, d), BF16), pltpu.SemaphoreType.DMA((SOURCES,))],
        ),
        cost_estimate=cost(6 * rows * d * ff, 8 * d * ff),
        compiler_params=pltpu.CompilerParams(vmem_limit_bytes=VMEM_LIMIT),
        name="up_rest",
    )(num, *sources, pos, near, wg, wu)


def down_kernel(num, begin, one_ref, two_ref, mix, w_ref, *refs):
    outs, (h, out, acc, sems) = refs[:SOURCES], refs[SOURCES:]
    e, j = pl.program_id(0), pl.program_id(1)
    window = mix.shape[2]
    columns = pl.ds(pl.multiple_of(j * DOWN_BLOCK, DOWN_BLOCK), DOWN_BLOCK)
    start = (e == 0) & (j == 0)

    def load(k, c, t):
        at = pl.ds(pl.multiple_of(t * c, 32), c)
        return pltpu.make_async_copy((one_ref, two_ref)[k].at[at], h.at[k, at], sems.at[k, t])

    @pl.when(start)
    def _():
        out[...] = jnp.zeros_like(out)

    @pl.when((e == 0) & (j == 1))
    def _():
        def body(c, n):
            load(1, c, 0).start()
            pl.when(n > 1)(lambda: load(1, c, 1).start())

        chunks_do(num[ROWS + 1], body)

    def body(c, n):
        pl.when(start)(lambda: load(0, c, 0).start())

        def chunk(t, _):
            @pl.when(start)
            def _():
                load(0, c, t).wait()
                pl.when(t + 1 < n)(lambda: load(0, c, t + 1).start())

            pl.when((e == 1) & (j == 0))(lambda: load(1, c, t).wait())
            at = pl.ds(pl.multiple_of(t * c, 32), c)
            out[at] = jnp.dot(h[e, at], w_ref[...], preferred_element_type=F32).astype(BF16)
            return 0

        lax.fori_loop(0, n, chunk, 0)

    chunks_do(num[ROWS + e], body)

    def term(s):
        low = pl.multiple_of(floor16(num[START + 8 * e + s]), 16)
        return jnp.dot(mix[e * SOURCES + s], out[pl.ds(low, window)], preferred_element_type=F32)

    @pl.when(e == 0)
    def _():
        for s in range(SOURCES):
            acc[s, :, columns] = term(s)

    @pl.when(e == 1)
    def _():
        for s in range(SOURCES):
            outs[s][...] = (acc[s, :, columns] + term(s)).astype(outs[s].dtype)


def down(num, begin, one, two, mix, w, size):
    tokens, window = mix.shape[1:]
    rows, ff = two.shape
    weights = pl.BlockSpec(
        (None, ff, DOWN_BLOCK), lambda e, j, num, begin: (num[FIRST + e], 0, begin[0] + j)
    )
    return pl.pallas_call(
        down_kernel,
        out_shape=[jax.ShapeDtypeStruct((tokens, size), F32 if s == 0 else BF16) for s in range(SOURCES)],
        grid_spec=pltpu.PrefetchScalarGridSpec(
            num_scalar_prefetch=2,
            grid=(2, size // DOWN_BLOCK),
            in_specs=[pl.BlockSpec(memory_space=pl.ANY)] * 2
            + [pl.BlockSpec(mix.shape, lambda e, j, num, begin: (0, 0, 0), pipeline_mode=pl.Buffered(1)), weights],
            out_specs=[pl.BlockSpec((tokens, DOWN_BLOCK), lambda e, j, num, begin: (0, e * j))] * SOURCES,
            scratch_shapes=[
                pltpu.VMEM((2, rows, ff), BF16),
                pltpu.VMEM((rows + window, DOWN_BLOCK), BF16),
                pltpu.VMEM((SOURCES, tokens, size), F32),
                pltpu.SemaphoreType.DMA((2, 2)),
            ],
        ),
        cost_estimate=cost(4 * rows * ff * size, 4 * ff * size + 4 * rows * ff),
        compiler_params=pltpu.CompilerParams(vmem_limit_bytes=VMEM_LIMIT),
        name="down",
    )(num, begin, one, two, mix, w)


def solution(mesh):
    members = mesh.shape["ep"]

    def swap(v, code):
        pairs = [(i, i ^ code) for i in range(2 * members)]
        return lax.ppermute(v, ("dp", "ep"), pairs)

    def layer(x, expert, slot, gate, w_gate, w_up, w_down):
        x, expert, slot, gate = x[0, 0], expert[0, 0], slot[0, 0], gate[0, 0]
        tokens, top = expert.shape
        slots = 5 * tokens * top // (4 * members * w_gate.shape[0])
        pos, scale, num = plan(expert.T, slot.T, gate.T, slots)
        num = num.reshape(128)
        mate = swap(x, 1)
        x, num = lax.optimization_barrier((x, num))
        far, across = swap(x, 2), swap(x, 4)
        near, mix = up_near(num, x, mate, pos, scale, w_gate, w_up, slots)
        far, across, near = lax.optimization_barrier((far, across, near))
        sources = (x, mate, far, swap(far, 1), across, swap(across, 1))
        one, two = up_rest(num, sources, pos, near, w_gate, w_up, slots)
        parts, start = [], 0
        for size in CHUNKS:
            y, *send = down(num, jnp.full((1,), start // DOWN_BLOCK, I32), one, two, mix, w_down, size)
            got = [swap(term, s + 1) for s, term in enumerate(send)]
            for term in got:
                y = y + term.astype(F32)
            parts.append(y.astype(BF16))
            start += size
        return jnp.concatenate(parts, 1)[None, None]

    tokens_spec = P("dp", "ep", None, None)
    weight_spec = P("ep", None, None)
    return jax.shard_map(
        layer,
        mesh=mesh,
        in_specs=(tokens_spec,) * 4 + (weight_spec,) * 3,
        out_specs=tokens_spec,
        check_vma=False,
    )
```

```python
import functools

import jax
import jax.numpy as jnp
from jax import lax
from jax.experimental import pallas as pl
from jax.experimental.pallas import tpu as pltpu
from jax.sharding import PartitionSpec as P


F32, BF16, I32 = jnp.float32, jnp.bfloat16, jnp.int32
MESH = pl.DeviceIdType.MESH
VMEM_LIMIT = 62 * 2**20
CHUNKS = (2560, 2048, 1536)
NEAR_BLOCK, REST_BLOCK, DOWN_BLOCK = 512, 512, 256
NEAR_ROWS = 160
NEAR_STEPS = 15
ROW_CHUNKS = (192, 224, 256, 288, 320)
SOURCES = 6
FIRST, SECOND, NEAR, ROWS, START, COUNT = 0, 1, 2, 3, 8, 24


def cost(flops, nbytes):
    return pl.CostEstimate(flops=int(flops), bytes_accessed=int(nbytes), transcendentals=0)


def plan_kernel(slots, expert_ref, slot_ref, gate_ref, pos_ref, scale_ref, num_ref, mine, got, send, recv):
    dp, ep = lax.axis_index("dp"), lax.axis_index("ep")
    tokens = expert_ref.shape[1]

    def peer(i):
        return (dp ^ (i // 4), ep ^ (i % 4))

    expert, slot = expert_ref[...], slot_ref[...]
    gate = gate_ref[...].astype(BF16).astype(F32)
    for pair in range(4):
        rows = []
        for e in (2 * pair, 2 * pair + 1):
            hit = (expert == e) & (slot < slots)
            rows.append(jnp.sum(jnp.where(hit, 1.0, 0.0), 0, keepdims=True))
            rows.append(jnp.sum(jnp.where(hit, gate, 0.0), 0, keepdims=True))
        rows = [rows[0], rows[2], rows[1], rows[3], jnp.zeros((4, tokens), F32)]
        mine[pair] = jnp.concatenate(rows, 0)

    barrier = pltpu.get_barrier_semaphore()
    for i in range(1, 8):
        pl.semaphore_signal(barrier, inc=1, device_id=peer(i), device_id_type=MESH)
    pl.semaphore_wait(barrier, 7)
    copies = []
    for i in range(1, 8):
        copies.append(
            pltpu.make_async_remote_copy(
                src_ref=mine.at[ep ^ (i % 4)],
                dst_ref=got.at[i],
                send_sem=send.at[i],
                recv_sem=recv.at[i],
                device_id=peer(i),
                device_id_type=MESH,
            )
        )
    for copy in copies:
        copy.start()
    for copy in copies:
        copy.wait()

    blocks = [mine[ep]] + [got[i] for i in range(1, 8)]
    valid = jnp.concatenate([b[0:2] for b in blocks], 0)
    scales = [b[2:4] for b in blocks]
    upper = lax.broadcasted_iota(I32, (tokens, tokens), 0) <= lax.broadcasted_iota(I32, (tokens, tokens), 1)
    upto = jnp.dot(valid.astype(BF16), upper.astype(F32).astype(BF16), preferred_element_type=F32)

    results = []
    for e in range(2):
        v = [valid[2 * i + e : 2 * i + e + 1] > 0.0 for i in range(8)]
        rank = [upto[2 * i + e : 2 * i + e + 1] - 1.0 for i in range(8)]
        c = [r[:, tokens - 1 :] + 1.0 for r in rank]
        near, other = c[0] + c[1], c[4] + c[5]
        gap = near + c[2] + c[3] - other - c[6] - c[7]
        give = jnp.minimum(jnp.maximum(jnp.floor(gap * 0.5), 0.0), near)
        take = jnp.minimum(jnp.maximum(jnp.floor(-gap * 0.5), 0.0), other)
        keep, skip = near - give, other - take
        counts = [jnp.minimum(c[0], keep)]
        counts += [keep - counts[0], c[2], c[3], jnp.maximum(c[4] - skip, 0.0)]
        counts += [take - counts[4]]
        starts = [jnp.zeros_like(keep)]
        for n in counts:
            starts.append(starts[-1] + n)
        place = [rank[0], rank[1] + c[0], rank[2] + starts[2], rank[3] + starts[3]]
        mine_too = [v[0] & (place[0] < keep), v[1] & (place[1] < keep), v[2], v[3]]
        for i, n in ((4, rank[4]), (5, rank[5] + c[4])):
            mine_too.append(v[i] & (n >= skip))
            place.append(n - skip + starts[4])
        pos = [jnp.where(m, p, -1.0) for m, p in zip(mine_too, place)]
        results.append((keep, starts[6], starts[:6], counts, pos, [s[e : e + 1] for s in scales[:6]]))

    swap = results[1][0] > results[0][0]

    def pick(a, b):
        return jnp.where(swap, b, a), jnp.where(swap, a, b)

    (a_keep, a_rows, a_starts, a_counts, a_pos, a_scale), (b_keep, b_rows, b_starts, b_counts, b_pos, b_scale) = results
    pad = jnp.full((2, tokens), -1.0, F32)
    pos = [pick(a, b) for a, b in zip(a_pos, b_pos)]
    scale = [pick(a, b) for a, b in zip(a_scale, b_scale)]
    pos_ref[...] = jnp.concatenate([p[0] for p in pos] + [pad] + [p[1] for p in pos] + [pad], 0).astype(I32)
    scale_ref[...] = jnp.concatenate([p[0] for p in scale] + [pad] + [p[1] for p in scale] + [pad], 0)
    lane = lax.broadcasted_iota(I32, (1, 128), 1)
    numbers = {FIRST: jnp.where(swap, 1.0, 0.0), SECOND: jnp.where(swap, 0.0, 1.0)}
    numbers[NEAR] = pick(a_keep, b_keep)[0]
    numbers[ROWS], numbers[ROWS + 1] = pick(a_rows, b_rows)
    for s in range(SOURCES):
        numbers[START + s], numbers[START + 8 + s] = pick(a_starts[s], b_starts[s])
        numbers[COUNT + s], numbers[COUNT + 8 + s] = pick(a_counts[s], b_counts[s])
    out = jnp.zeros((1, 128), F32)
    for at, value in numbers.items():
        out = jnp.where(lane == at, value, out)
    num_ref[...] = out.astype(I32)


def plan(expert, slot, gate, slots):
    tokens = expert.shape[1]
    return pl.pallas_call(
        functools.partial(plan_kernel, slots),
        out_shape=[
            jax.ShapeDtypeStruct((16, tokens), I32),
            jax.ShapeDtypeStruct((16, tokens), F32),
            jax.ShapeDtypeStruct((1, 128), I32),
        ],
        scratch_shapes=[
            pltpu.VMEM((4, 8, tokens), F32),
            pltpu.VMEM((8, 8, tokens), F32),
            pltpu.SemaphoreType.DMA((8,)),
            pltpu.SemaphoreType.DMA((8,)),
        ],
        cost_estimate=cost(10**7, 10**5),
        compiler_params=pltpu.CompilerParams(collective_id=0, has_side_effects=True),
        name="plan",
    )(expert, slot, gate)


def floor16(n):
    return n // 16 * 16


def place_rows(window, x_ref, pos, start, count, z_ref, block=2048):
    tokens, d = x_ref.shape
    low = pl.multiple_of(floor16(start), 16)

    @pl.when(count > 0)
    def _():
        rows = lax.broadcasted_iota(I32, (window, tokens), 0) + low
        pick = (rows == pos).astype(F32).astype(BF16)

        def step(k, _):
            at = pl.ds(pl.multiple_of(k * block, block), block)
            z = jnp.dot(pick, x_ref[:, at], preferred_element_type=F32).astype(BF16)
            z_ref[pl.ds(low, window), at] += z
            return 0

        lax.fori_loop(0, d // block, step, 0)


def chunks_do(rows, body):
    single = [c for c in ROW_CHUNKS if c % 64 == 0]
    for c in ROW_CHUNKS:
        two = (rows > max(2 * c - 64, ROW_CHUNKS[-1])) & (rows <= 2 * c)
        use = two
        if c in single:
            k = single.index(c)
            use = two | ((rows > (single[k - 1] if k else -1)) & (rows <= c))
        pl.when(use)(functools.partial(body, c, jnp.where(two, 2, 1)))


def swiglu(z, wg, wu):
    g = jnp.dot(z, wg, preferred_element_type=F32)
    u = jnp.dot(z, wu, preferred_element_type=F32)
    return (jax.nn.silu(g) * u).astype(BF16)


def up_near_kernel(window, num, x_ref, mate_ref, pos_ref, scale_ref, wg_ref, wu_ref, h_ref, mix_ref, z):
    j = pl.program_id(0)
    tokens = x_ref.shape[0]

    @pl.when((j > 0) & (j <= 2 * SOURCES))
    def _():
        k = j - 1
        row = k // SOURCES * 8 + lax.rem(k, SOURCES)
        at = lax.broadcasted_iota(I32, (window, tokens), 0) + floor16(num[START + row])
        weight = jnp.where(at == pos_ref[pl.ds(row, 1), :], scale_ref[pl.ds(row, 1), :], 0.0)
        mix_ref[k] = weight.T.astype(BF16)

    @pl.when(j == 0)
    def _():
        z[...] = jnp.zeros_like(z)
        for s, ref in enumerate((x_ref, mate_ref)):
            place_rows(window, ref, pos_ref[s : s + 1, :], num[START + s], num[COUNT + s], z)

    two = num[NEAR] > NEAR_ROWS

    @pl.when(jnp.logical_not(two))
    def _():
        h_ref[NEAR_ROWS:] = jnp.zeros((NEAR_ROWS, h_ref.shape[1]), BF16)

    def chunk(t, _):
        at = pl.ds(pl.multiple_of(t * NEAR_ROWS, 32), NEAR_ROWS)
        h_ref[at] = swiglu(z[at], wg_ref[...], wu_ref[...])
        return 0

    lax.fori_loop(0, jnp.where(two, 2, 1), chunk, 0)


def up_near(num, x, mate, pos, scale, wg, wu, slots):
    tokens, d = x.shape
    window, rows = slots + 16, 2 * NEAR_ROWS
    whole = pl.BlockSpec((tokens, d), lambda j, num: (0, 0), pipeline_mode=pl.Buffered(1))
    weights = pl.BlockSpec((None, d, NEAR_BLOCK), lambda j, num: (num[FIRST], 0, j))
    return pl.pallas_call(
        functools.partial(up_near_kernel, window),
        out_shape=[
            jax.ShapeDtypeStruct((rows, NEAR_STEPS * NEAR_BLOCK), BF16),
            jax.ShapeDtypeStruct((2 * SOURCES, tokens, window), BF16),
        ],
        grid_spec=pltpu.PrefetchScalarGridSpec(
            num_scalar_prefetch=1,
            grid=(NEAR_STEPS,),
            in_specs=[whole, whole]
            + [pl.BlockSpec(pos.shape, lambda j, num: (0, 0))] * 2
            + [weights, weights],
            out_specs=[
                pl.BlockSpec((rows, NEAR_BLOCK), lambda j, num: (0, j)),
                pl.BlockSpec((2 * SOURCES, tokens, window), lambda j, num: (0, 0, 0)),
            ],
            scratch_shapes=[pltpu.VMEM((rows + window, d), BF16)],
        ),
        cost_estimate=cost(4 * rows * d * NEAR_STEPS * NEAR_BLOCK, 4 * d * NEAR_STEPS * NEAR_BLOCK),
        compiler_params=pltpu.CompilerParams(vmem_limit_bytes=VMEM_LIMIT),
        name="up_near",
    )(num, x, mate, pos, scale, wg, wu)


def up_rest_kernel(window, steps, num, *refs):
    sources, (pos_ref, near_ref, wg_ref, wu_ref, one_ref, two_ref), xs = (
        refs[:SOURCES],
        refs[SOURCES : SOURCES + 6],
        refs[SOURCES + 6 : 2 * SOURCES + 6],
    )
    z, sems = refs[2 * SOURCES + 6 :]
    j = pl.program_id(0)
    copies = [pltpu.make_async_copy(sources[s], xs[s], sems.at[s]) for s in range(SOURCES)]

    order = (2, 4, 3, 5, 0, 1)

    @pl.when(j == 0)
    def _():
        for s in order[:2]:
            copies[s].start()

    @pl.when((j == 0) | (j == steps))
    def _():
        z[...] = jnp.zeros_like(z)
        for k, s in enumerate(order):

            @pl.when(j == 0)
            def _():
                copies[s].wait()
                if k + 2 < SOURCES:
                    copies[order[k + 2]].start()

            row = jnp.where(j == 0, s, 8 + s)
            place_rows(window, xs[s], pos_ref[pl.ds(row, 1), :], num[START + row], num[COUNT + row], z)

    near_rows = near_ref.shape[0]
    first = j < steps
    base = jnp.where(j < NEAR_STEPS, floor16(num[NEAR]), 0)
    rows = jnp.where(first, num[ROWS] - base, num[ROWS + 1])

    @pl.when(first)
    def _():
        one_ref[0:near_rows] = near_ref[...]
        one_ref[near_rows:] = jnp.zeros((one_ref.shape[0] - near_rows, one_ref.shape[1]), BF16)

    @pl.when(jnp.logical_not(first))
    def _():
        two_ref[...] = jnp.zeros_like(two_ref)

    def body(c, n):
        def chunk(t, _):
            at = pl.ds(pl.multiple_of(base + t * c, 16), c)
            h = swiglu(z[at], wg_ref[...], wu_ref[...])

            @pl.when(first)
            def _():
                one_ref[at] = h

            @pl.when(jnp.logical_not(first))
            def _():
                two_ref[at] = h

            return 0

        lax.fori_loop(0, n, chunk, 0)

    chunks_do(rows, body)


def up_rest(num, sources, pos, near, wg, wu, slots):
    tokens, d = sources[0].shape
    ff = wg.shape[2]
    window, rows = slots + 16, 2 * ROW_CHUNKS[-1]
    steps = ff // REST_BLOCK
    weights = pl.BlockSpec(
        (None, d, REST_BLOCK),
        lambda j, num: (jnp.where(j < steps, num[FIRST], num[SECOND]), 0, lax.rem(j, steps)),
    )
    early = lambda j, num: (0, jnp.minimum(j, steps - 1))
    late = lambda j, num: (0, jnp.maximum(j - steps, 0))
    return pl.pallas_call(
        functools.partial(up_rest_kernel, window, steps),
        out_shape=[jax.ShapeDtypeStruct((rows + 128, ff), BF16), jax.ShapeDtypeStruct((rows, ff), BF16)],
        grid_spec=pltpu.PrefetchScalarGridSpec(
            num_scalar_prefetch=1,
            grid=(2 * steps,),
            in_specs=[pl.BlockSpec(memory_space=pl.ANY)] * SOURCES
            + [
                pl.BlockSpec(pos.shape, lambda j, num: (0, 0)),
                pl.BlockSpec((near.shape[0], REST_BLOCK), lambda j, num: (0, jnp.minimum(j, NEAR_STEPS - 1))),
                weights,
                weights,
            ],
            out_specs=[pl.BlockSpec((rows + 128, REST_BLOCK), early), pl.BlockSpec((rows, REST_BLOCK), late)],
            scratch_shapes=[pltpu.VMEM((tokens, d), BF16)] * SOURCES
            + [pltpu.VMEM((rows + window, d), BF16), pltpu.SemaphoreType.DMA((SOURCES,))],
        ),
        cost_estimate=cost(6 * rows * d * ff, 8 * d * ff),
        compiler_params=pltpu.CompilerParams(vmem_limit_bytes=VMEM_LIMIT),
        name="up_rest",
    )(num, *sources, pos, near, wg, wu)


def down_kernel(num, begin, one_ref, two_ref, mix, w_ref, *refs):
    outs, (h, out, acc, sems) = refs[:SOURCES], refs[SOURCES:]
    e, j = pl.program_id(0), pl.program_id(1)
    window = mix.shape[2]
    columns = pl.ds(pl.multiple_of(j * DOWN_BLOCK, DOWN_BLOCK), DOWN_BLOCK)
    start = (e == 0) & (j == 0)

    def load(k, c, t):
        at = pl.ds(pl.multiple_of(t * c, 32), c)
        return pltpu.make_async_copy((one_ref, two_ref)[k].at[at], h.at[k, at], sems.at[k, t])

    @pl.when(start)
    def _():
        out[...] = jnp.zeros_like(out)

    @pl.when((e == 0) & (j == 1))
    def _():
        def body(c, n):
            load(1, c, 0).start()
            pl.when(n > 1)(lambda: load(1, c, 1).start())

        chunks_do(num[ROWS + 1], body)

    def body(c, n):
        pl.when(start)(lambda: load(0, c, 0).start())

        def chunk(t, _):
            @pl.when(start)
            def _():
                load(0, c, t).wait()
                pl.when(t + 1 < n)(lambda: load(0, c, t + 1).start())

            pl.when((e == 1) & (j == 0))(lambda: load(1, c, t).wait())
            at = pl.ds(pl.multiple_of(t * c, 32), c)
            out[at] = jnp.dot(h[e, at], w_ref[...], preferred_element_type=F32).astype(BF16)
            return 0

        lax.fori_loop(0, n, chunk, 0)

    chunks_do(num[ROWS + e], body)

    def term(s):
        low = pl.multiple_of(floor16(num[START + 8 * e + s]), 16)
        return jnp.dot(mix[e * SOURCES + s], out[pl.ds(low, window)], preferred_element_type=F32)

    @pl.when(e == 0)
    def _():
        for s in range(SOURCES):
            acc[s, :, columns] = term(s)

    @pl.when(e == 1)
    def _():
        for s in range(SOURCES):
            outs[s][...] = (acc[s, :, columns] + term(s)).astype(outs[s].dtype)


def down(num, begin, one, two, mix, w, size):
    tokens, window = mix.shape[1:]
    rows, ff = two.shape
    weights = pl.BlockSpec(
        (None, ff, DOWN_BLOCK), lambda e, j, num, begin: (num[FIRST + e], 0, begin[0] + j)
    )
    return pl.pallas_call(
        down_kernel,
        out_shape=[jax.ShapeDtypeStruct((tokens, size), F32 if s == 0 else BF16) for s in range(SOURCES)],
        grid_spec=pltpu.PrefetchScalarGridSpec(
            num_scalar_prefetch=2,
            grid=(2, size // DOWN_BLOCK),
            in_specs=[pl.BlockSpec(memory_space=pl.ANY)] * 2
            + [pl.BlockSpec(mix.shape, lambda e, j, num, begin: (0, 0, 0), pipeline_mode=pl.Buffered(1)), weights],
            out_specs=[pl.BlockSpec((tokens, DOWN_BLOCK), lambda e, j, num, begin: (0, e * j))] * SOURCES,
            scratch_shapes=[
                pltpu.VMEM((2, rows, ff), BF16),
                pltpu.VMEM((rows + window, DOWN_BLOCK), BF16),
                pltpu.VMEM((SOURCES, tokens, size), F32),
                pltpu.SemaphoreType.DMA((2, 2)),
            ],
        ),
        cost_estimate=cost(4 * rows * ff * size, 4 * ff * size + 4 * rows * ff),
        compiler_params=pltpu.CompilerParams(vmem_limit_bytes=VMEM_LIMIT),
        name="down",
    )(num, begin, one, two, mix, w)


def solution(mesh):
    members = mesh.shape["ep"]

    def swap(v, code):
        pairs = [(i, i ^ code) for i in range(2 * members)]
        return lax.ppermute(v, ("dp", "ep"), pairs)

    def layer(x, expert, slot, gate, w_gate, w_up, w_down):
        x, expert, slot, gate = x[0, 0], expert[0, 0], slot[0, 0], gate[0, 0]
        tokens, top = expert.shape
        slots = 5 * tokens * top // (4 * members * w_gate.shape[0])
        pos, scale, num = plan(expert.T, slot.T, gate.T, slots)
        num = num.reshape(128)
        mate = swap(x, 1)
        x, num = lax.optimization_barrier((x, num))
        far, across = swap(x, 2), swap(x, 4)
        near, mix = up_near(num, x, mate, pos, scale, w_gate, w_up, slots)
        far, across, near = lax.optimization_barrier((far, across, near))
        sources = (x, mate, far, swap(far, 1), across, swap(across, 1))
        one, two = up_rest(num, sources, pos, near, w_gate, w_up, slots)
        parts, start = [], 0
        for size in CHUNKS:
            y, *send = down(num, jnp.full((1,), start // DOWN_BLOCK, I32), one, two, mix, w_down, size)
            got = [swap(term, s + 1) for s, term in enumerate(send)]
            for term in got:
                y = y + term.astype(F32)
            parts.append(y.astype(BF16))
            start += size
        return jnp.concatenate(parts, 1)[None, None]

    tokens_spec = P("dp", "ep", None, None)
    weight_spec = P("ep", None, None)
    return jax.shard_map(
        layer,
        mesh=mesh,
        in_specs=(tokens_spec,) * 4 + (weight_spec,) * 3,
        out_specs=tokens_spec,
        check_vma=False,
    )
```
